32 devices in a mesh: rows: 4 (over z), rhs: 8 (over y, x, core).
Axes of the slice: x: 2, y: 2, z: 4, core: 2. Of those that a mesh axis runs over, the one named last changes fastest.
Arguments:
- rhs_blocks: bfloat16 [4, 2048, 1024], P('rows', None, 'rhs'), may hold values from -6 to 6
- left_u: bfloat16 [4, 4, 2048, 256], P('rows', None, 'rhs'), may hold values from -0.375 to 0.375
- left_v: bfloat16 [4, 4, 2048, 256], P('rows', None, 'rhs'), may hold values from -0.125 to 0.125
- tile_ranks: int32 [4, 4], P('rows'), may hold values from 32 to 256
- diag_inverse: bfloat16 [4, 2048, 2048], P(None, 'rows'), may hold values from -8 to 8, as said below
- row_owner: int32 [4], replicated, may hold values from 0 to 3, each once
Outputs:
- solved: bfloat16 [4, 2048, 1024], P(None, 'rows', 'rhs')
- updated: bfloat16 [4, 2048, 1024], P('rows', None, 'rhs')
The draws below stay inside these ranges and needn't reach their ends.
Inputs may be any that keep to these rules, and one draw needn't show every extreme that they name: tile_ranks[s, k] is the rank of the tile in column k of the tile row stored in block s. row_owner[s] is the tile row held in stored block s; every tile row is held exactly once. Each diag_inverse[k] is lower triangular.
All inputs are finite; a program needn't handle non-finite values.
Results may differ from the reference program's by a relative error of at most 0.01.
Values may be sent and summed in bfloat16 or wider, within the bound.
No kernel may reach another device: no remote copies, remote signals or barrier semaphores. Data moves between devices by JAX's collectives and lax.ppermute only.
A program may use at most 64 MiB of HBM per device.

```python
import jax
import jax.numpy as jnp
from jax import lax

TS = 2048
RMAX = 256
WIN = 4
NT = 4
NRHS = 1024


def draw_diag_inverse(key, part):
    first_key, second_key = jax.random.split(jax.random.fold_in(key, 17))
    lower = jnp.tril(jnp.ones((TS, TS), jnp.float32), -1)
    off_diag = jax.random.normal(first_key, (WIN, TS, TS), jnp.float32)
    diagonal = jnp.exp(jax.random.uniform(second_key, (WIN, TS), jnp.float32, jnp.log(0.5), jnp.log(2.0)))
    eye_mat = jnp.eye(TS, dtype=jnp.float32)
    whole = off_diag * lower * TS ** (-0.5) + diagonal[:, :, None] * eye_mat
    return whole.astype(jnp.bfloat16)


def place_ends(array, stream_key, smallest, top_value):
    shape = array.shape
    place = [jax.random.randint(jax.random.fold_in(stream_key, axis), (), 0, shape[axis]) for axis in range(len(shape))]
    array = array.at[tuple(place)].set(smallest)
    longest = shape.index(max(shape))
    place[longest] = (place[longest] + 1) % shape[longest]
    return array.at[tuple(place)].set(top_value)


def block_levels(rng, extent, pieces, least, high):
    level, own = 1.0, jax.random.fold_in(rng, 6)
    for axis_at, blocks in pieces:
        heights = jnp.exp(jax.random.uniform(jax.random.fold_in(own, axis_at), (blocks,), jnp.float32, least / len(pieces), high / len(pieces)))
        level = level * jnp.repeat(heights, extent[axis_at] // blocks).reshape([-1 if axis == axis_at else 1 for axis in range(len(extent))])
    return level


def scatter_about(key, shape, scale, reach, cuts=(), held_as=jnp.bfloat16):
    drawn = scale * jax.random.normal(key, shape, jnp.float32)
    if cuts:
        drawn = drawn * block_levels(key, shape, cuts, -0.22, 0.18)
    return jnp.clip(drawn, -reach, reach).astype(held_as)


def setup_inputs(seed: int = 0) -> dict:
    splits = jax.random.split(jax.random.key(seed), 7)
    rhs_blocks = scatter_about(splits[0], (NT, TS, NRHS), 1.0, 6.0, ((0, 4), (2, 8)))
    left_u = scatter_about(splits[1], (NT, WIN, TS, RMAX), RMAX ** -0.5, 0.375, ((0, 4), (2, 8)))
    left_v = scatter_about(splits[2], (NT, WIN, TS, RMAX), TS ** -0.5, 0.125, ((0, 4), (2, 8)))
    tile_ranks = place_ends(jax.random.randint(splits[3], (NT, WIN), RMAX // 8, RMAX + 1), jax.random.fold_in(splits[3], 1), RMAX // 8, RMAX).astype(jnp.int32)
    diag_inverse = draw_diag_inverse(jax.random.fold_in(splits[6], 71), 0)
    row_owner = jax.random.permutation(splits[5], NT).astype(jnp.int32)
    return {"rhs_blocks": rhs_blocks, "left_u": left_u, "left_v": left_v, "tile_ranks": tile_ranks, "diag_inverse": diag_inverse, "row_owner": row_owner}


def reference(rhs_blocks, left_u, left_v, tile_ranks, diag_inverse, row_owner):
    residual = rhs_blocks.astype(jnp.float32)
    stored = jnp.arange(NT, dtype=jnp.int32)
    solved_list = []
    for column in range(WIN):
        owner_index = jnp.sum(jnp.where(row_owner == column, stored, 0)).astype(jnp.int32)
        next_rows = lax.dynamic_index_in_dim(residual, owner_index, 0, keepdims=False).astype(jnp.bfloat16)
        solution = jnp.dot(diag_inverse[column], next_rows, preferred_element_type=jnp.float32).astype(jnp.bfloat16)
        solved_list.append(solution)

        def apply_tile(items):
            u_tile, v_tile, tile_rank, owner_row, old_rows = items
            keep_cols = (jnp.arange(RMAX, dtype=jnp.int32) < tile_rank).astype(v_tile.dtype)
            coeffs = jnp.dot((v_tile * keep_cols).T, solution, preferred_element_type=jnp.float32).astype(jnp.bfloat16)
            update = jnp.dot(u_tile, coeffs, preferred_element_type=jnp.float32)
            return jnp.where(column < owner_row, old_rows - update, old_rows)

        residual = lax.map(apply_tile, (left_u[:, column], left_v[:, column], tile_ranks[:, column], row_owner, residual))
    return jnp.stack(solved_list), residual.astype(jnp.bfloat16)
```

```python
import functools

import jax
import jax.numpy as jnp
from jax import lax
from jax.experimental import pallas as pl
from jax.experimental.pallas import tpu as pltpu
from jax.sharding import PartitionSpec as P

F32, BF16 = jnp.float32, jnp.bfloat16


def left_product(v_piece, x_rows, tile_rank):
    width = v_piece.shape[1]
    keep_cols = (jnp.arange(width, dtype=jnp.int32) < tile_rank).astype(v_piece.dtype)
    dims = (((0,), (0,)), ((), ()))
    return lax.dot_general(v_piece * keep_cols, x_rows, dims, preferred_element_type=F32)


def right_product(u_piece, coeffs):
    return jnp.dot(u_piece, coeffs, preferred_element_type=F32)


def general_body(rhs_blocks, left_u, left_v, tile_ranks, diag_inverse, row_owner):
    my_index = lax.axis_index("rows")
    stored = jnp.arange(row_owner.shape[0], dtype=jnp.int32)
    my_row = jnp.sum(jnp.where(stored == my_index, row_owner, 0))
    residual = rhs_blocks[0].astype(F32)
    solved_parts = []
    for column in range(diag_inverse.shape[0]):
        owner_index = jnp.sum(jnp.where(row_owner == column, stored, 0))
        rounded = residual.astype(BF16).astype(F32)
        offered = jnp.where(my_index == owner_index, rounded, jnp.zeros_like(rounded))
        own_piece = lax.psum_scatter(offered.astype(BF16), "rows", scatter_dimension=0, tiled=True)
        solved_part = jnp.dot(
            diag_inverse[column],
            lax.all_gather(own_piece, "rows", axis=0, tiled=True),
            preferred_element_type=F32,
        ).astype(BF16)
        solved_parts.append(solved_part)
        solution = lax.all_gather(solved_part, "rows", axis=0, tiled=True)
        coeffs = left_product(
            lax.all_gather(left_v[0, column], "rhs", axis=0, tiled=True), solution, tile_ranks[0, column]
        ).astype(BF16)
        update = right_product(lax.all_gather(left_u[0, column], "rhs", axis=0, tiled=True), coeffs)
        residual = jnp.where(column < my_row, residual - update, residual)
    return (jnp.stack(solved_parts), residual.astype(BF16)[None])


PLACES = ((0, None), (2, None), (4, None), (1, None), (6, 0), (6, 1), (3, None), (5, None), (7, 0), (7, 1))


def gather_lanes(block):
    def swap(array, bit):
        return lax.ppermute(array, "rhs", [(i, i ^ bit) for i in range(8)])

    half = block.shape[1] // 2
    over_x, over_y, partner = swap(block, 2), swap(block, 4), swap(block, 1)
    far_lo, far_hi = swap(over_x[:, :half], 4), swap(over_y[:, half:], 2)
    rest = [swap(piece, 1) for piece in (over_x, over_y, far_lo, far_hi)]
    return [block, over_x, over_y, partner, far_lo, far_hi, *rest]


def rows_of(ref, place, lane, rows):
    k, half = place
    start = jnp.bitwise_xor(lane, k) * rows
    count = rows if half is None else rows // 2
    if half:
        start = start + count
    return pl.multiple_of(start, count), count


def apply_update(column, n_rows, meta, residual, coeff_refs, u_refs, coeff):
    me, lane = meta[meta.shape[0] - 2], meta[meta.shape[0] - 1]
    mine = meta[me]
    owner = sum(jnp.where(meta[s] == column, s, 0) for s in range(n_rows))
    shift = lax.rem(owner - me + n_rows, n_rows)
    rank = meta[n_rows + column]

    @pl.when(column < mine)
    def _():
        for delta in range(1, n_rows):

            @pl.when(shift == delta)
            def _():
                coeff[...] = coeff_refs[delta - 1][...]

        cols = lax.broadcasted_iota(jnp.int32, coeff.shape, 1)
        kept = jnp.where(cols < rank, coeff[...].astype(F32), 0.0).astype(BF16)
        for place, u_ref in zip(PLACES, u_refs):
            whole = u_ref.shape[1] if place[1] is None else 2 * u_ref.shape[1]
            first, count = rows_of(u_ref, place, lane, whole)
            update = lax.dot_general(
                u_ref[0], kept, (((1,), (1,)), ((), ())), preferred_element_type=F32
            )
            residual[pl.ds(first, count), :] = residual[pl.ds(first, count), :] - update


def step_kernel(column, n_rows, n_u, meta, start, *refs):
    refs = list(refs)
    take = lambda n: [refs.pop(0) for _ in range(n)]
    coeff_refs, u_refs = take(n_rows - 1 if column else 0), take(n_u)
    (own_diag,), diag_refs, v_refs = take(1), take(10), take(10)
    before = take(1) if column else []
    (residual, solved), out_coeffs = take(2), take(n_rows - 1)
    (coeff,) = take(1)
    me, lane = meta[meta.shape[0] - 2], meta[meta.shape[0] - 1]
    mine = meta[me]
    residual[...] = start[...].astype(F32)
    if column:
        apply_update(column - 1, n_rows, meta, residual, coeff_refs, u_refs, coeff)

        @pl.when(mine < column)
        def _():
            solved[...] = before[0][...]

    @pl.when(mine == column)
    def _():
        rounded = residual[...].astype(BF16)
        piece = own_diag.shape[0]
        rows = piece // 8
        solved[pl.ds(pl.multiple_of(me * piece, piece), piece), :] = jnp.dot(
            own_diag[...], rounded, preferred_element_type=F32
        ).astype(BF16)
        for place, ref in zip(PLACES, diag_refs):
            first, count = rows_of(ref, place, lane, rows)
            product = jnp.dot(
                ref[...].reshape((n_rows - 1) * count, ref.shape[2]), rounded, preferred_element_type=F32
            ).astype(BF16)
            for delta in range(1, n_rows):
                source = lax.rem(me - delta + n_rows, n_rows)
                at = pl.multiple_of(source * piece + first, count)
                solved[pl.ds(at, count), :] = product[(delta - 1) * count : delta * count]
        for delta in range(1, n_rows):
            total = jnp.zeros(coeff.shape, F32)
            for place, ref in zip(PLACES, v_refs):
                whole = ref.shape[1] if place[1] is None else 2 * ref.shape[1]
                first, count = rows_of(ref, place, lane, whole)
                total += lax.dot_general(
                    solved[pl.ds(first, count), :],
                    ref[delta - 1],
                    (((0,), (0,)), ((), ())),
                    preferred_element_type=F32,
                )
            out_coeffs[delta - 1][...] = total.astype(BF16)


def last_kernel(column, n_rows, meta, start, *refs):
    coeff_refs, u_refs = refs[: n_rows - 1], refs[n_rows - 1 : n_rows + 9]
    residual, coeff = refs[n_rows + 9 :]
    residual[...] = start[...]
    apply_update(column, n_rows, meta, residual, coeff_refs, u_refs, coeff)


VMEM = pl.BlockSpec(memory_space=pltpu.VMEM)
SMEM = pl.BlockSpec(memory_space=pltpu.SMEM)


def body(rhs_blocks, left_u, left_v, tile_ranks, diag_inverse, row_owner):
    n_cols, piece, order = diag_inverse.shape
    n_rows = row_owner.shape[0]
    width, rank_max = rhs_blocks.shape[2], left_u.shape[3]
    rows = piece // 8
    me, lane = lax.axis_index("rows"), lax.axis_index("rhs")
    meta = jnp.concatenate([row_owner, tile_ranks[0], jnp.stack([me, lane]).astype(jnp.int32)])

    def shifted(array, delta):
        return lax.ppermute(array, "rows", [(i, (i + delta) % n_rows) for i in range(n_rows)])

    def column_of(stored):
        return jnp.minimum(jnp.sum(jnp.where(jnp.arange(n_rows) == stored, row_owner, 0)), n_cols - 1)

    own_diag = lax.dynamic_index_in_dim(diag_inverse, column_of(me), 0, keepdims=False)
    diag_got, v_got = [], []
    for delta in range(1, n_rows):
        target = column_of((me + delta) % n_rows)
        rows_out = lax.dynamic_slice(diag_inverse, (target, lane * rows, 0), (1, rows, order))
        diag_got.append(shifted(rows_out, delta))
        v_got.append(shifted(lax.dynamic_index_in_dim(left_v[0], target, 0), delta))
    u_all = [gather_lanes(left_u[0, k : k + 1]) for k in range(min(n_cols, n_rows - 1))]
    v_all = gather_lanes(jnp.concatenate(v_got))
    diag_all = gather_lanes(jnp.concatenate(diag_got))

    residual, solved, got = rhs_blocks[0], None, []
    shapes = [jax.ShapeDtypeStruct((order, width), F32), jax.ShapeDtypeStruct((order, width), BF16)]
    shapes += [jax.ShapeDtypeStruct((width, rank_max), BF16)] * (n_rows - 1)
    scratch = [pltpu.VMEM((width, rank_max), BF16)]
    for column in range(n_cols):
        u_now = u_all[column - 1] if column else []
        operands = [meta, residual, *got, *u_now, own_diag, *diag_all, *v_all]
        if column:
            operands.append(solved)
        residual, solved, *coeffs = pl.pallas_call(
            functools.partial(step_kernel, column, n_rows, len(u_now)),
            out_shape=shapes,
            in_specs=[SMEM] + [VMEM] * (len(operands) - 1),
            out_specs=[VMEM] * len(shapes),
            scratch_shapes=scratch,
            name=f"step_{column}",
        )(*operands)
        if column < n_rows - 1:
            got = [shifted(c, n_rows - delta) for delta, c in zip(range(1, n_rows), coeffs)]

    def finish(residual, got, u_now):
        return pl.pallas_call(
            functools.partial(last_kernel, n_cols - 1, n_rows),
            out_shape=shapes[0],
            in_specs=[SMEM] + [VMEM] * (1 + len(got) + len(u_now)),
            out_specs=VMEM,
            scratch_shapes=scratch,
            name="last_update",
        )(meta, residual, *got, *u_now)

    if n_cols < n_rows:
        residual = finish(residual, got, u_all[n_cols - 1])
    else:

        def with_last(operands):
            residual, coeffs, u_last = operands
            got = [shifted(c, n_rows - delta) for delta, c in zip(range(1, n_rows), coeffs)]
            return finish(residual, got, gather_lanes(u_last))

        residual = lax.cond(
            jnp.max(row_owner) > n_cols - 1,
            with_last,
            lambda operands: operands[0],
            (residual, coeffs, left_u[0, n_cols - 1 :]),
        )
    pieces = lax.all_to_all(solved.reshape(n_rows, piece, width), "rows", 0, 0)
    owners = [jnp.sum(jnp.where(row_owner == j, jnp.arange(n_rows), 0)) for j in range(n_cols)]
    solved_out = jnp.stack([lax.dynamic_index_in_dim(pieces, s, 0, keepdims=False) for s in owners])
    return solved_out, residual.astype(BF16)[None]


def solution(mesh):
    direct = mesh.shape["rhs"] == 2**3 and mesh.shape["rows"] <= 4
    return jax.shard_map(
        body if direct else general_body,
        mesh=mesh,
        in_specs=(
            P("rows", None, "rhs"),
            P("rows", None, "rhs", None),
            P("rows", None, "rhs", None),
            P("rows", None),
            P(None, "rows", None),
            P(),
        ),
        out_specs=(P(None, "rows", "rhs"), P("rows", None, "rhs")),
        check_vma=False,
    )
```

```python
import functools

import jax
import jax.numpy as jnp
from jax import lax
from jax.experimental import pallas as pl
from jax.experimental.pallas import tpu as pltpu
from jax.sharding import PartitionSpec as P


F32, BF16 = jnp.float32, jnp.bfloat16


def left_product(v_piece, x_rows, tile_rank):
    width = v_piece.shape[1]
    keep_cols = (jnp.arange(width, dtype=jnp.int32) < tile_rank).astype(v_piece.dtype)
    dims = (((0,), (0,)), ((), ()))
    return lax.dot_general(v_piece * keep_cols, x_rows, dims, preferred_element_type=F32)


def right_product(u_piece, coeffs):
    return jnp.dot(u_piece, coeffs, preferred_element_type=F32)


def general_body(rhs_blocks, left_u, left_v, tile_ranks, diag_inverse, row_owner):
    my_index = lax.axis_index("rows")
    stored = jnp.arange(row_owner.shape[0], dtype=jnp.int32)
    my_row = jnp.sum(jnp.where(stored == my_index, row_owner, 0))
    residual = rhs_blocks[0].astype(F32)
    solved_parts = []
    for column in range(diag_inverse.shape[0]):
        owner_index = jnp.sum(jnp.where(row_owner == column, stored, 0))
        rounded = residual.astype(BF16).astype(F32)
        offered = jnp.where(my_index == owner_index, rounded, jnp.zeros_like(rounded))
        own_piece = lax.psum_scatter(offered.astype(BF16), "rows", scatter_dimension=0, tiled=True)
        solved_part = jnp.dot(
            diag_inverse[column],
            lax.all_gather(own_piece, "rows", axis=0, tiled=True),
            preferred_element_type=F32,
        ).astype(BF16)
        solved_parts.append(solved_part)
        solution = lax.all_gather(solved_part, "rows", axis=0, tiled=True)
        coeffs = left_product(
            lax.all_gather(left_v[0, column], "rhs", axis=0, tiled=True), solution, tile_ranks[0, column]
        ).astype(BF16)
        update = right_product(lax.all_gather(left_u[0, column], "rhs", axis=0, tiled=True), coeffs)
        residual = jnp.where(column < my_row, residual - update, residual)
    return (jnp.stack(solved_parts), residual.astype(BF16)[None])


PLACES = ((0, 1, 2, 3, 6, 5, 4, 7), (0, 1, 4, 5, 6, 3, 2, 7))


def gather_lanes(block):
    across = [(i, i ^ (4 if i & 1 else 2)) for i in range(8)]
    onward = [(i, i ^ (2 if i & 1 else 4)) for i in range(8)]
    swap = [(i, i ^ 1) for i in range(8)]
    near = lax.ppermute(block, "rhs", across)
    partner = lax.ppermute(block, "rhs", swap)
    near_partner = lax.ppermute(partner, "rhs", across)
    far = lax.ppermute(near, "rhs", onward)
    rest = [lax.ppermute(piece, "rhs", swap) for piece in (near, near_partner)]
    return [block, partner, near, near_partner, far, *rest]


def gather_rest(got, after=None):
    far = got[4]
    if after is not None:
        far = lax.optimization_barrier((far, after))[0]
    return [*got, lax.ppermute(far, "rhs", [(i, i ^ 1) for i in range(8)])]


def first_row(n, lane, rows):
    offset = jnp.where(lane & 1 == 0, PLACES[0][n], PLACES[1][n])
    return pl.multiple_of(jnp.bitwise_xor(lane, offset) * rows, rows)


def position():
    return lax.axis_index("rows"), lax.axis_index("rhs")


def around(index, n_rows):
    return lax.rem(index + n_rows, n_rows)


def pack_kernel(n_rows, owner, diag, left_v, left_u, *refs):
    packed, (u_out, tiles, sems) = refs[: n_rows - 1], refs[n_rows - 1 :]
    me, lane = position()
    n_cols, piece = diag.shape[0], diag.shape[1]
    rows, half = piece // 8, tiles.shape[1] // 2
    moves, tile_moves = [], []

    def move(source, target):
        copy = pltpu.make_async_copy(source, target, sems.at[len(moves) + len(tile_moves)])
        copy.start()
        return copy

    for delta, out in enumerate(packed, 1):
        column = jnp.minimum(owner[around(me + delta - n_rows, n_rows)], n_cols - 1)
        tile_moves.append(move(left_v.at[0, column], tiles.at[delta - 1]))
        for b in range(n_rows):
            share = pl.ds(pl.multiple_of(lane * rows, rows), rows)
            source = diag.at[column, share, pl.ds(b * piece, piece)]
            moves.append(move(source, out.at[pl.ds(b * rows, rows), :]))
    moves.append(move(left_u.at[0, pl.ds(0, u_out.shape[0])], u_out))
    for delta, out in enumerate(packed):
        tile_moves[delta].wait()
        turned = tiles[delta].T
        out[n_rows * rows :, : 2 * half] = turned[:half]
        out[n_rows * rows :, 2 * half :] = turned[half:]
    for copy in moves:
        copy.wait()


def keep_kernel(owner, diag, rhs, own_diag, rhs_out, sems):
    column = jnp.minimum(owner[position()[0]], diag.shape[0] - 1)
    moves = [
        pltpu.make_async_copy(diag.at[column], own_diag, sems.at[0]),
        pltpu.make_async_copy(rhs.at[0], rhs_out, sems.at[1]),
    ]
    for copy in moves:
        copy.start()
    for copy in moves:
        copy.wait()


def apply_update(column, n_rows, owner, ranks, residual, coeff_refs, u_refs, coeff, slot):
    me, lane = position()
    holder = sum(jnp.where(owner[s] == column, s, 0) for s in range(n_rows))
    shift = around(holder - me, n_rows)
    rank = ranks[0, column]

    @pl.when(column < owner[me])
    def _():
        for delta in range(1, n_rows):

            @pl.when(shift == delta)
            def _():
                index = lax.broadcasted_iota(jnp.int32, coeff.shape, 0)
                coeff[...] = jnp.where(index < rank, coeff_refs[delta - 1][...].astype(F32), 0.0).astype(BF16)

        for n, u_ref in enumerate(u_refs):
            at = pl.ds(first_row(n, lane, u_ref.shape[1]), u_ref.shape[1])
            update = jnp.dot(u_ref[slot], coeff[...], preferred_element_type=F32)
            residual[at, :] = residual[at, :] - update


def write_coefficients(n_rows, solved, packed_refs, out_coeffs):
    lane = position()[1]
    rank_max = out_coeffs[0].shape[0]
    total = 0.0
    for n in range(8):
        parts = []
        for delta in range(n_rows - 1):
            turned = packed_refs[8 * delta + n][-rank_max // 2 :, :]
            parts += [turned[:, : turned.shape[1] // 2], turned[:, turned.shape[1] // 2 :]]
        factor = jnp.concatenate(parts)
        at = pl.ds(first_row(n, lane, factor.shape[1]), factor.shape[1])
        total += jnp.dot(factor, solved[at, :], preferred_element_type=F32)
    for delta, out in enumerate(out_coeffs):
        out[...] = total[delta * rank_max : (delta + 1) * rank_max].astype(BF16)


def step_kernel(column, last, n_rows, owner, ranks, start, *refs):
    refs = list(refs)
    take = lambda n: [refs.pop(0) for _ in range(n)]
    coeff_refs, u_refs, before = [], [], []
    if column:
        coeff_refs, u_refs, before = take(n_rows - 1), take(8), take(n_rows)
    (own_diag,), packed_refs = take(1), take(8 * (n_rows - 1))
    chunks = take(n_rows)
    (residual, *out_coeffs), refs = ([refs[-1]], refs[:-1]) if last else (refs[:n_rows], refs[n_rows:])
    solved, products, coeff = refs
    me, lane = position()
    mine = owner[me]
    residual[...] = start[...].astype(F32)
    if column:
        apply_update(column - 1, n_rows, owner, ranks, residual, coeff_refs, u_refs, coeff, column - 1)

        @pl.when(mine < column)
        def _():
            for chunk, earlier in zip(chunks, before):
                chunk[...] = earlier[...]

    @pl.when(mine == column)
    def _():
        piece = own_diag.shape[0]
        rows = piece // 8
        for block in range(n_rows):
            at = slice(block * piece, (block + 1) * piece)
            rounded = residual[at, :].astype(BF16)
            for delta in range(n_rows):
                source = around(me - delta, n_rows)

                @pl.when(source >= block)
                def _():
                    if delta:
                        refs_of = packed_refs[8 * (delta - 1) : 8 * delta]
                        sent = jnp.concatenate([ref[block * rows : (block + 1) * rows, :] for ref in refs_of])
                    else:
                        sent = own_diag[:, at]
                    product = jnp.dot(sent, rounded, preferred_element_type=F32)
                    products[delta] = products[delta] + product if block else product

        for delta in range(n_rows):
            base = around(me - delta, n_rows) * piece
            whole = products[delta].astype(BF16)
            if delta:
                for n in range(8):
                    at = pl.multiple_of(base + first_row(n, lane, rows), rows)
                    solved[pl.ds(at, rows), :] = whole[n * rows : (n + 1) * rows]
            else:
                solved[pl.ds(pl.multiple_of(base, piece), piece), :] = whole
        for delta, chunk in enumerate(chunks):
            target = around(me + delta - n_rows, n_rows)
            chunk[...] = solved[pl.ds(pl.multiple_of(target * piece, piece), piece), :]
        if not last:
            write_coefficients(n_rows, solved, packed_refs, out_coeffs)


def coefficient_kernel(n_rows, owner, ranks, *refs):
    n_packed = 8 * (n_rows - 1)
    chunks, packed_refs, out_coeffs = refs[:n_rows], refs[n_rows : n_rows + n_packed], refs[n_rows + n_packed : -1]
    solved = refs[-1]
    for delta, chunk in enumerate(chunks):
        piece = chunk.shape[0]
        target = around(position()[0] + delta - n_rows, n_rows)
        solved[pl.ds(pl.multiple_of(target * piece, piece), piece), :] = chunk[...]
    write_coefficients(n_rows, solved, packed_refs, out_coeffs)


def last_kernel(column, slot, n_rows, owner, ranks, start, *refs):
    coeff_refs, u_refs = refs[: n_rows - 1], refs[n_rows - 1 : n_rows + 7]
    residual, updated, coeff = refs[n_rows + 7 :]
    residual[...] = start[...]
    apply_update(column, n_rows, owner, ranks, residual, coeff_refs, u_refs, coeff, slot)
    updated[...] = residual[...].astype(BF16)


def place_kernel(n_rows, owner, ranks, *refs):
    chunks, (out,) = refs[:n_rows], refs[n_rows:]
    for delta, chunk in enumerate(chunks):
        column = owner[around(position()[0] - delta, n_rows)]

        @pl.when(column < out.shape[0])
        def _():
            out[column] = chunk[...]


VMEM = pl.BlockSpec(memory_space=pltpu.VMEM)
SMEM = pl.BlockSpec(memory_space=pltpu.SMEM)


def body(rhs_blocks, left_u, left_v, tile_ranks, diag_inverse, row_owner):
    return direct_body(rhs_blocks, left_u, left_v, tile_ranks, diag_inverse, row_owner)


def direct_body(rhs_blocks, left_u, left_v, tile_ranks, diag_inverse, row_owner):
    n_cols, piece, order = diag_inverse.shape
    n_rows = row_owner.shape[0]
    width, rank_max = rhs_blocks.shape[2], left_u.shape[3]
    rows = piece // 8
    n_u = min(n_cols, n_rows - 1)

    def shifted(array, delta):
        return lax.ppermute(array, "rows", [(i, (i + delta) % n_rows) for i in range(n_rows)])

    def like(*shape):
        return jax.ShapeDtypeStruct(shape, BF16)

    chunk = left_u.shape[2]
    anywhere = pl.BlockSpec(memory_space=pl.ANY)
    *packed, u_mine = pl.pallas_call(
        functools.partial(pack_kernel, n_rows),
        out_shape=[like(n_rows * rows + rank_max // 2, piece)] * (n_rows - 1) + [like(n_u, chunk, rank_max)],
        in_specs=[SMEM] + [anywhere] * 3,
        out_specs=[VMEM] * n_rows,
        scratch_shapes=[
            pltpu.VMEM((n_rows - 1, chunk, rank_max), BF16),
            pltpu.SemaphoreType.DMA(((n_rows - 1) * (n_rows + 1) + 1,)),
        ],
        compiler_params=pltpu.CompilerParams(vmem_limit_bytes=52 * 2**20),
        name="pack",
    )(row_owner, diag_inverse, left_v, left_u)
    own_diag, residual = pl.pallas_call(
        keep_kernel,
        out_shape=[like(piece, order), like(order, width)],
        in_specs=[SMEM, anywhere, anywhere],
        out_specs=[VMEM] * 2,
        scratch_shapes=[pltpu.SemaphoreType.DMA((2,))],
        compiler_params=pltpu.CompilerParams(vmem_limit_bytes=48 * 2**20),
        name="keep",
    )(row_owner, diag_inverse, rhs_blocks)
    packed[1], own_diag, residual = lax.optimization_barrier((packed[1], own_diag, residual))
    u_all = gather_lanes(u_mine)
    packed_all = []
    for delta in range(1, n_rows):
        packed_all += gather_rest(gather_lanes(shifted(packed[delta - 1], delta)))

    whole, halved = jax.ShapeDtypeStruct((order, width), F32), jax.ShapeDtypeStruct((order, width), BF16)
    chunk_shapes = [jax.ShapeDtypeStruct((piece, width), BF16)] * n_rows
    coeff_shapes = [like(rank_max, width)] * (n_rows - 1)
    coeff_scratch = pltpu.VMEM((rank_max, width), BF16)
    params = pltpu.CompilerParams(vmem_limit_bytes=26 * 2**20)

    def call(kernel, in_specs, out_shape, scratch, *operands):
        return pl.pallas_call(
            kernel,
            out_shape=out_shape,
            in_specs=[SMEM, SMEM] + in_specs,
            out_specs=[VMEM] * len(out_shape) if isinstance(out_shape, list) else VMEM,
            scratch_shapes=scratch,
            compiler_params=params,
            cost_estimate=pl.CostEstimate(flops=2 * order * order * width, bytes_accessed=0, transcendentals=0),
        )(row_owner, tile_ranks, *operands)

    def sent_back(coeffs):
        pairs = zip(range(1, n_rows), coeffs)
        return [shifted(c, n_rows - delta) for delta, c in pairs]

    chunks, coeffs = [], []
    scratch = [pltpu.VMEM((order, width), BF16), pltpu.VMEM((n_rows, piece, width), F32), coeff_scratch]
    for column in range(n_cols):
        last = column == n_cols - 1
        if column == 1:
            u_all = gather_rest(u_all, residual)
        before = [*sent_back(coeffs), *u_all, *chunks] if column else []
        outs = call(
            functools.partial(step_kernel, column, last, n_rows),
            [VMEM] * (2 + len(before) + len(packed_all)),
            chunk_shapes + ([] if last else [whole] + coeff_shapes),
            scratch + ([pltpu.VMEM((order, width), F32)] if last else []),
            residual, *before, own_diag, *packed_all,
        )
        chunks, rest = outs[:n_rows], outs[n_rows:]
        if not last:
            residual, coeffs = rest[0], rest[1:]
    arrived = [chunks[0]] + [shifted(chunks[delta], delta) for delta in range(1, n_rows)]
    residual, updated = call(
        functools.partial(last_kernel, n_cols - 2, n_cols - 2, n_rows),
        [VMEM] * (n_rows + 8), [whole, halved], [coeff_scratch], residual, *before[: n_rows + 7],
    )

    def finish(residual, _, chunks, u_last, packed_all):
        coeffs = call(
            functools.partial(coefficient_kernel, n_rows),
            [VMEM] * (n_rows + len(packed_all)), coeff_shapes, scratch[:1], *chunks, *packed_all,
        )
        got, u_all = sent_back(coeffs), gather_rest(gather_lanes(u_last))
        return call(
            functools.partial(last_kernel, n_cols - 1, 0, n_rows),
            [VMEM] * (n_rows + 8), [whole, halved], [coeff_scratch], residual, *got, *u_all,
        )[1]

    updated = lax.cond(
        jnp.max(row_owner) > n_cols - 1,
        finish,
        lambda _, updated, *rest: updated,
        residual, updated, chunks, left_u[0, n_cols - 1 :], packed_all,
    )
    solved_out = call(
        functools.partial(place_kernel, n_rows),
        [VMEM] * n_rows, jax.ShapeDtypeStruct((n_cols, piece, width), BF16), [], *arrived,
    )
    return solved_out, updated[None]


def solution(mesh):
    direct = mesh.shape["rhs"] == 2**3 and mesh.shape["rows"] == 2**2
    return jax.shard_map(
        body if direct else general_body,
        mesh=mesh,
        in_specs=(
            P("rows", None, "rhs"),
            P("rows", None, "rhs", None),
            P("rows", None, "rhs", None),
            P("rows", None),
            P(None, "rows", None),
            P(),
        ),
        out_specs=(P(None, "rows", "rhs"), P("rows", None, "rhs")),
        check_vma=False,
    )
```

```python
import functools

import jax
import jax.numpy as jnp
from jax import lax
from jax.experimental import pallas as pl
from jax.experimental.pallas import tpu as pltpu
from jax.sharding import PartitionSpec as P


F32, BF16 = jnp.float32, jnp.bfloat16


def left_product(v_piece, x_rows, tile_rank):
    width = v_piece.shape[1]
    keep_cols = (jnp.arange(width, dtype=jnp.int32) < tile_rank).astype(v_piece.dtype)
    dims = (((0,), (0,)), ((), ()))
    return lax.dot_general(v_piece * keep_cols, x_rows, dims, preferred_element_type=F32)


def right_product(u_piece, coeffs):
    return jnp.dot(u_piece, coeffs, preferred_element_type=F32)


def general_body(rhs_blocks, left_u, left_v, tile_ranks, diag_inverse, row_owner):
    my_index = lax.axis_index("rows")
    stored = jnp.arange(row_owner.shape[0], dtype=jnp.int32)
    my_row = jnp.sum(jnp.where(stored == my_index, row_owner, 0))
    residual = rhs_blocks[0].astype(F32)
    solved_parts = []
    for column in range(diag_inverse.shape[0]):
        owner_index = jnp.sum(jnp.where(row_owner == column, stored, 0))
        rounded = residual.astype(BF16).astype(F32)
        offered = jnp.where(my_index == owner_index, rounded, jnp.zeros_like(rounded))
        own_piece = lax.psum_scatter(offered.astype(BF16), "rows", scatter_dimension=0, tiled=True)
        solved_part = jnp.dot(
            diag_inverse[column],
            lax.all_gather(own_piece, "rows", axis=0, tiled=True),
            preferred_element_type=F32,
        ).astype(BF16)
        solved_parts.append(solved_part)
        solution = lax.all_gather(solved_part, "rows", axis=0, tiled=True)
        coeffs = left_product(
            lax.all_gather(left_v[0, column], "rhs", axis=0, tiled=True), solution, tile_ranks[0, column]
        ).astype(BF16)
        update = right_product(lax.all_gather(left_u[0, column], "rhs", axis=0, tiled=True), coeffs)
        residual = jnp.where(column < my_row, residual - update, residual)
    return (jnp.stack(solved_parts), residual.astype(BF16)[None])


PLACES = ((0, 1, 2, 3, 6, 5, 4, 7), (0, 1, 4, 5, 6, 3, 2, 7))


def gather_lanes(block):
    across = [(i, i ^ (4 if i & 1 else 2)) for i in range(8)]
    onward = [(i, i ^ (2 if i & 1 else 4)) for i in range(8)]
    swap = [(i, i ^ 1) for i in range(8)]
    near = lax.ppermute(block, "rhs", across)
    partner = lax.ppermute(block, "rhs", swap)
    near_partner = lax.ppermute(partner, "rhs", across)
    far = lax.ppermute(near, "rhs", onward)
    rest = [lax.ppermute(piece, "rhs", swap) for piece in (near, near_partner)]
    return [block, partner, near, near_partner, far, *rest]


def gather_rest(got, after=None):
    far = got[4]
    if after is not None:
        far = lax.optimization_barrier((far, after))[0]
    return [*got, lax.ppermute(far, "rhs", [(i, i ^ 1) for i in range(8)])]


def first_row(n, lane, rows):
    offset = jnp.where(lane & 1 == 0, PLACES[0][n], PLACES[1][n])
    return pl.multiple_of(jnp.bitwise_xor(lane, offset) * rows, rows)


def position():
    return lax.axis_index("rows"), lax.axis_index("rhs")


def around(index, n_rows):
    return lax.rem(index + n_rows, n_rows)


def pack_kernel(n_rows, owner, diag, left_v, left_u, *refs):
    packed, (u_out, tiles, sems) = refs[: n_rows - 1], refs[n_rows - 1 :]
    me, lane = position()
    n_cols, piece = diag.shape[0], diag.shape[1]
    rows, half = piece // 8, tiles.shape[1] // 2
    moves, tile_moves = [], []

    def move(source, target):
        copy = pltpu.make_async_copy(source, target, sems.at[len(moves) + len(tile_moves)])
        copy.start()
        return copy

    for delta, out in enumerate(packed, 1):
        column = jnp.minimum(owner[around(me + delta - n_rows, n_rows)], n_cols - 1)
        tile_moves.append(move(left_v.at[0, column], tiles.at[delta - 1]))
        for b in range(n_rows):
            share = pl.ds(pl.multiple_of(lane * rows, rows), rows)
            source = diag.at[column, share, pl.ds(b * piece, piece)]
            moves.append(move(source, out.at[pl.ds(b * rows, rows), :]))
    moves.append(move(left_u.at[0, pl.ds(0, u_out.shape[0])], u_out))
    for delta, out in enumerate(packed):
        tile_moves[delta].wait()
        turned = tiles[delta].T
        out[n_rows * rows :, : 2 * half] = turned[:half]
        out[n_rows * rows :, 2 * half :] = turned[half:]
    for copy in moves:
        copy.wait()


def keep_kernel(owner, diag, rhs, own_diag, rhs_out, sems):
    column = jnp.minimum(owner[position()[0]], diag.shape[0] - 1)
    moves = [
        pltpu.make_async_copy(diag.at[column], own_diag, sems.at[0]),
        pltpu.make_async_copy(rhs.at[0], rhs_out, sems.at[1]),
    ]
    for copy in moves:
        copy.start()
    for copy in moves:
        copy.wait()


def apply_update(column, n_rows, owner, ranks, residual, coeff_refs, u_refs, coeff, slot):
    me, lane = position()
    holder = sum(jnp.where(owner[s] == column, s, 0) for s in range(n_rows))
    shift = around(holder - me, n_rows)
    rank = ranks[0, column]

    @pl.when(column < owner[me])
    def _():
        for delta in range(1, n_rows):

            @pl.when(shift == delta)
            def _():
                index = lax.broadcasted_iota(jnp.int32, coeff.shape, 0)
                coeff[...] = jnp.where(index < rank, coeff_refs[delta - 1][...].astype(F32), 0.0).astype(BF16)

        for n, u_ref in enumerate(u_refs):
            at = pl.ds(first_row(n, lane, u_ref.shape[1]), u_ref.shape[1])
            update = jnp.dot(u_ref[slot], coeff[...], preferred_element_type=F32)
            residual[at, :] = residual[at, :] - update


def write_coefficients(n_rows, solved, packed_refs, out_coeffs):
    lane = position()[1]
    rank_max = out_coeffs[0].shape[0]
    total = 0.0
    for n in range(8):
        parts = []
        for delta in range(n_rows - 1):
            turned = packed_refs[8 * delta + n][-rank_max // 2 :, :]
            parts += [turned[:, : turned.shape[1] // 2], turned[:, turned.shape[1] // 2 :]]
        factor = jnp.concatenate(parts)
        at = pl.ds(first_row(n, lane, factor.shape[1]), factor.shape[1])
        total += jnp.dot(factor, solved[at, :], preferred_element_type=F32)
    for delta, out in enumerate(out_coeffs):
        out[...] = total[delta * rank_max : (delta + 1) * rank_max].astype(BF16)


def step_kernel(column, last, n_rows, owner, ranks, start, *refs):
    refs = list(refs)
    take = lambda n: [refs.pop(0) for _ in range(n)]
    coeff_refs, u_refs, before = [], [], []
    if column:
        coeff_refs, u_refs, before = take(n_rows - 1), take(8), take(n_rows)
    (own_diag,), packed_refs = take(1), take(8 * (n_rows - 1))
    chunks = take(n_rows)
    (residual, *out_coeffs), refs = ([refs[-1]], refs[:-1]) if last else (refs[:n_rows], refs[n_rows:])
    solved, products, coeff = refs
    me, lane = position()
    mine = owner[me]
    residual[...] = start[...].astype(F32)
    if column:
        apply_update(column - 1, n_rows, owner, ranks, residual, coeff_refs, u_refs, coeff, column - 1)

        @pl.when(mine < column)
        def _():
            for chunk, earlier in zip(chunks, before):
                chunk[...] = earlier[...]

    @pl.when(mine == column)
    def _():
        piece = own_diag.shape[0]
        rows = piece // 8
        rounded = residual[...].astype(BF16)
        half = n_rows // 2

        def product(delta, first):
            at = slice(first * piece, (first + half) * piece)
            if not delta:
                return jnp.dot(own_diag[:, at], rounded[at], preferred_element_type=F32)
            blocks = range(first, first + half)
            sent = [
                jnp.concatenate([ref[b * rows : (b + 1) * rows, :] for b in blocks], axis=1)
                for ref in packed_refs[8 * (delta - 1) : 8 * delta]
            ]
            return jnp.dot(jnp.concatenate(sent), rounded[at], preferred_element_type=F32)

        for delta in range(n_rows):
            products[delta] = product(delta, 0)
        for delta in range(n_rows):

            @pl.when(around(me - delta, n_rows) >= half)
            def _():
                products[delta] = products[delta] + product(delta, half)

        for delta in range(n_rows):
            base = around(me - delta, n_rows) * piece
            whole = products[delta].astype(BF16)
            if delta:
                for n in range(8):
                    at = pl.multiple_of(base + first_row(n, lane, rows), rows)
                    solved[pl.ds(at, rows), :] = whole[n * rows : (n + 1) * rows]
            else:
                solved[pl.ds(pl.multiple_of(base, piece), piece), :] = whole
        for delta, chunk in enumerate(chunks):
            target = around(me + delta - n_rows, n_rows)
            chunk[...] = solved[pl.ds(pl.multiple_of(target * piece, piece), piece), :]
        if not last:
            write_coefficients(n_rows, solved, packed_refs, out_coeffs)


def coefficient_kernel(n_rows, owner, ranks, *refs):
    n_packed = 8 * (n_rows - 1)
    chunks, packed_refs, out_coeffs = refs[:n_rows], refs[n_rows : n_rows + n_packed], refs[n_rows + n_packed : -1]
    solved = refs[-1]
    for delta, chunk in enumerate(chunks):
        piece = chunk.shape[0]
        target = around(position()[0] + delta - n_rows, n_rows)
        solved[pl.ds(pl.multiple_of(target * piece, piece), piece), :] = chunk[...]
    write_coefficients(n_rows, solved, packed_refs, out_coeffs)


def last_kernel(column, slot, n_rows, owner, ranks, start, *refs):
    coeff_refs, u_refs = refs[: n_rows - 1], refs[n_rows - 1 : n_rows + 7]
    residual, updated, coeff = refs[n_rows + 7 :]
    residual[...] = start[...]
    apply_update(column, n_rows, owner, ranks, residual, coeff_refs, u_refs, coeff, slot)
    updated[...] = residual[...].astype(BF16)


def place_kernel(n_rows, owner, ranks, *refs):
    chunks, (out,) = refs[:n_rows], refs[n_rows:]
    for delta, chunk in enumerate(chunks):
        column = owner[around(position()[0] - delta, n_rows)]

        @pl.when(column < out.shape[0])
        def _():
            out[column] = chunk[...]


VMEM = pl.BlockSpec(memory_space=pltpu.VMEM)
SMEM = pl.BlockSpec(memory_space=pltpu.SMEM)


def body(rhs_blocks, left_u, left_v, tile_ranks, diag_inverse, row_owner):
    return direct_body(rhs_blocks, left_u, left_v, tile_ranks, diag_inverse, row_owner)


def direct_body(rhs_blocks, left_u, left_v, tile_ranks, diag_inverse, row_owner):
    n_cols, piece, order = diag_inverse.shape
    n_rows = row_owner.shape[0]
    width, rank_max = rhs_blocks.shape[2], left_u.shape[3]
    rows = piece // 8
    n_u = min(n_cols, n_rows - 1)

    def shifted(array, delta):
        return lax.ppermute(array, "rows", [(i, (i + delta) % n_rows) for i in range(n_rows)])

    def like(*shape):
        return jax.ShapeDtypeStruct(shape, BF16)

    chunk = left_u.shape[2]
    anywhere = pl.BlockSpec(memory_space=pl.ANY)
    *packed, u_mine = pl.pallas_call(
        functools.partial(pack_kernel, n_rows),
        out_shape=[like(n_rows * rows + rank_max // 2, piece)] * (n_rows - 1) + [like(n_u, chunk, rank_max)],
        in_specs=[SMEM] + [anywhere] * 3,
        out_specs=[VMEM] * n_rows,
        scratch_shapes=[
            pltpu.VMEM((n_rows - 1, chunk, rank_max), BF16),
            pltpu.SemaphoreType.DMA(((n_rows - 1) * (n_rows + 1) + 1,)),
        ],
        compiler_params=pltpu.CompilerParams(vmem_limit_bytes=52 * 2**20),
        name="pack",
    )(row_owner, diag_inverse, left_v, left_u)
    own_diag, residual = pl.pallas_call(
        keep_kernel,
        out_shape=[like(piece, order), like(order, width)],
        in_specs=[SMEM, anywhere, anywhere],
        out_specs=[VMEM] * 2,
        scratch_shapes=[pltpu.SemaphoreType.DMA((2,))],
        compiler_params=pltpu.CompilerParams(vmem_limit_bytes=48 * 2**20),
        name="keep",
    )(row_owner, diag_inverse, rhs_blocks)
    packed[1], own_diag, residual = lax.optimization_barrier((packed[1], own_diag, residual))
    u_all = gather_lanes(u_mine)
    packed_all = []
    for delta in range(1, n_rows):
        packed_all += gather_rest(gather_lanes(shifted(packed[delta - 1], delta)))

    whole, halved = jax.ShapeDtypeStruct((order, width), F32), jax.ShapeDtypeStruct((order, width), BF16)
    chunk_shapes = [jax.ShapeDtypeStruct((piece, width), BF16)] * n_rows
    coeff_shapes = [like(rank_max, width)] * (n_rows - 1)
    coeff_scratch = pltpu.VMEM((rank_max, width), BF16)
    params = pltpu.CompilerParams(vmem_limit_bytes=26 * 2**20)

    def call(kernel, in_specs, out_shape, scratch, *operands):
        return pl.pallas_call(
            kernel,
            out_shape=out_shape,
            in_specs=[SMEM, SMEM] + in_specs,
            out_specs=[VMEM] * len(out_shape) if isinstance(out_shape, list) else VMEM,
            scratch_shapes=scratch,
            compiler_params=params,
            cost_estimate=pl.CostEstimate(flops=2 * order * order * width, bytes_accessed=0, transcendentals=0),
        )(row_owner, tile_ranks, *operands)

    def sent_back(coeffs):
        pairs = zip(range(1, n_rows), coeffs)
        return [shifted(c, n_rows - delta) for delta, c in pairs]

    chunks, coeffs = [], []
    scratch = [pltpu.VMEM((order, width), BF16), pltpu.VMEM((n_rows, piece, width), F32), coeff_scratch]
    for column in range(n_cols):
        last = column == n_cols - 1
        if column == 1:
            u_all = gather_rest(u_all, residual)
        before = [*sent_back(coeffs), *u_all, *chunks] if column else []
        outs = call(
            functools.partial(step_kernel, column, last, n_rows),
            [VMEM] * (2 + len(before) + len(packed_all)),
            chunk_shapes + ([] if last else [whole] + coeff_shapes),
            scratch + ([pltpu.VMEM((order, width), F32)] if last else []),
            residual, *before, own_diag, *packed_all,
        )
        chunks, rest = outs[:n_rows], outs[n_rows:]
        if not last:
            residual, coeffs = rest[0], rest[1:]
    arrived = [chunks[0]] + [shifted(chunks[delta], delta) for delta in range(1, n_rows)]
    residual, updated = call(
        functools.partial(last_kernel, n_cols - 2, n_cols - 2, n_rows),
        [VMEM] * (n_rows + 8), [whole, halved], [coeff_scratch], residual, *before[: n_rows + 7],
    )

    def finish(residual, _, chunks, u_last, packed_all):
        coeffs = call(
            functools.partial(coefficient_kernel, n_rows),
            [VMEM] * (n_rows + len(packed_all)), coeff_shapes, scratch[:1], *chunks, *packed_all,
        )
        got, u_all = sent_back(coeffs), gather_rest(gather_lanes(u_last))
        return call(
            functools.partial(last_kernel, n_cols - 1, 0, n_rows),
            [VMEM] * (n_rows + 8), [whole, halved], [coeff_scratch], residual, *got, *u_all,
        )[1]

    updated = lax.cond(
        jnp.max(row_owner) > n_cols - 1,
        finish,
        lambda _, updated, *rest: updated,
        residual, updated, chunks, left_u[0, n_cols - 1 :], packed_all,
    )
    solved_out = call(
        functools.partial(place_kernel, n_rows),
        [VMEM] * n_rows, jax.ShapeDtypeStruct((n_cols, piece, width), BF16), [], *arrived,
    )
    return solved_out, updated[None]


def solution(mesh):
    direct = mesh.shape["rhs"] == 2**3 and mesh.shape["rows"] == 2**2
    return jax.shard_map(
        body if direct else general_body,
        mesh=mesh,
        in_specs=(
            P("rows", None, "rhs"),
            P("rows", None, "rhs", None),
            P("rows", None, "rhs", None),
            P("rows", None),
            P(None, "rows", None),
            P(),
        ),
        out_specs=(P(None, "rows", "rhs"), P("rows", None, "rhs")),
        check_vma=False,
    )
```

```python
import functools

import jax
import jax.numpy as jnp
from jax import lax
from jax.experimental import pallas as pl
from jax.experimental.pallas import tpu as pltpu
from jax.sharding import PartitionSpec as P


F32, BF16 = jnp.float32, jnp.bfloat16


def left_product(v_piece, x_rows, tile_rank):
    width = v_piece.shape[1]
    keep_cols = (jnp.arange(width, dtype=jnp.int32) < tile_rank).astype(v_piece.dtype)
    dims = (((0,), (0,)), ((), ()))
    return lax.dot_general(v_piece * keep_cols, x_rows, dims, preferred_element_type=F32)


def right_product(u_piece, coeffs):
    return jnp.dot(u_piece, coeffs, preferred_element_type=F32)


def general_body(rhs_blocks, left_u, left_v, tile_ranks, diag_inverse, row_owner):
    my_index = lax.axis_index("rows")
    stored = jnp.arange(row_owner.shape[0], dtype=jnp.int32)
    my_row = jnp.sum(jnp.where(stored == my_index, row_owner, 0))
    residual = rhs_blocks[0].astype(F32)
    solved_parts = []
    for column in range(diag_inverse.shape[0]):
        owner_index = jnp.sum(jnp.where(row_owner == column, stored, 0))
        rounded = residual.astype(BF16).astype(F32)
        offered = jnp.where(my_index == owner_index, rounded, jnp.zeros_like(rounded))
        own_piece = lax.psum_scatter(offered.astype(BF16), "rows", scatter_dimension=0, tiled=True)
        solved_part = jnp.dot(
            diag_inverse[column],
            lax.all_gather(own_piece, "rows", axis=0, tiled=True),
            preferred_element_type=F32,
        ).astype(BF16)
        solved_parts.append(solved_part)
        solution = lax.all_gather(solved_part, "rows", axis=0, tiled=True)
        coeffs = left_product(
            lax.all_gather(left_v[0, column], "rhs", axis=0, tiled=True), solution, tile_ranks[0, column]
        ).astype(BF16)
        update = right_product(lax.all_gather(left_u[0, column], "rhs", axis=0, tiled=True), coeffs)
        residual = jnp.where(column < my_row, residual - update, residual)
    return (jnp.stack(solved_parts), residual.astype(BF16)[None])


PLACES = ((0, 1, 2, 3, 6, 5, 4, 7), (0, 1, 4, 5, 6, 3, 2, 7))


def gather_lanes(block):
    across = [(i, i ^ (4 if i & 1 else 2)) for i in range(8)]
    onward = [(i, i ^ (2 if i & 1 else 4)) for i in range(8)]
    swap = [(i, i ^ 1) for i in range(8)]
    near = lax.ppermute(block, "rhs", across)
    partner = lax.ppermute(block, "rhs", swap)
    near_partner = lax.ppermute(partner, "rhs", across)
    far = lax.ppermute(near, "rhs", onward)
    rest = [lax.ppermute(piece, "rhs", swap) for piece in (near, near_partner)]
    return [block, partner, near, near_partner, far, *rest]


def gather_rest(got, after=None):
    far = got[4]
    if after is not None:
        far = lax.optimization_barrier((far, after))[0]
    return [*got, lax.ppermute(far, "rhs", [(i, i ^ 1) for i in range(8)])]


def first_row(n, lane, rows):
    offset = jnp.where(lane & 1 == 0, PLACES[0][n], PLACES[1][n])
    return pl.multiple_of(jnp.bitwise_xor(lane, offset) * rows, rows)


def position():
    return lax.axis_index("rows"), lax.axis_index("rhs")


def around(index, n_rows):
    return lax.rem(index + n_rows, n_rows)


def pack_kernel(n_rows, owner, diag, left_v, left_u, *refs):
    packed, (u_out, tiles, sems) = refs[: n_rows - 1], refs[n_rows - 1 :]
    me, lane = position()
    n_cols, piece = diag.shape[0], diag.shape[1]
    rows, half = piece // 8, tiles.shape[1] // 2
    moves, tile_moves = [], []

    def move(source, target):
        copy = pltpu.make_async_copy(source, target, sems.at[len(moves) + len(tile_moves)])
        copy.start()
        return copy

    for delta, out in enumerate(packed, 1):
        column = jnp.minimum(owner[around(me + delta - n_rows, n_rows)], n_cols - 1)
        tile_moves.append(move(left_v.at[0, column], tiles.at[delta - 1]))
        for b in range(n_rows):
            share = pl.ds(pl.multiple_of(lane * rows, rows), rows)
            source = diag.at[column, share, pl.ds(b * piece, piece)]
            moves.append(move(source, out.at[pl.ds(b * rows, rows), :]))
    moves.append(move(left_u.at[0, pl.ds(0, u_out.shape[0])], u_out))
    for delta, out in enumerate(packed):
        tile_moves[delta].wait()
        turned = tiles[delta].T
        out[n_rows * rows :, : 2 * half] = turned[:half]
        out[n_rows * rows :, 2 * half :] = turned[half:]
    for copy in moves:
        copy.wait()


def keep_kernel(owner, diag, rhs, own_diag, rhs_out, sems):
    column = jnp.minimum(owner[position()[0]], diag.shape[0] - 1)
    moves = [
        pltpu.make_async_copy(diag.at[column], own_diag, sems.at[0]),
        pltpu.make_async_copy(rhs.at[0], rhs_out, sems.at[1]),
    ]
    for copy in moves:
        copy.start()
    for copy in moves:
        copy.wait()


def apply_update(column, n_rows, owner, ranks, start, residual, coeff_refs, u_refs, coeff, slot):
    me, lane = position()
    holder = sum(jnp.where(owner[s] == column, s, 0) for s in range(n_rows))
    shift = around(holder - me, n_rows)
    rank = ranks[0, column]

    @pl.when(column < owner[me])
    def _():
        for delta in range(1, n_rows):

            @pl.when(shift == delta)
            def _():
                index = lax.broadcasted_iota(jnp.int32, coeff.shape, 0)
                coeff[...] = jnp.where(index < rank, coeff_refs[delta - 1][...].astype(F32), 0.0).astype(BF16)

        for n, u_ref in enumerate(u_refs):
            at = pl.ds(first_row(n, lane, u_ref.shape[1]), u_ref.shape[1])
            update = jnp.dot(u_ref[slot], coeff[...], preferred_element_type=F32)
            residual[at, :] = start[at, :] - update

    @pl.when(column >= owner[me])
    def _():
        residual[...] = start[...]


def write_coefficients(n_rows, solved, packed_refs, out_coeffs):
    lane = position()[1]
    rank_max = out_coeffs[0].shape[0]
    total = 0.0
    for n in range(8):
        parts = []
        for delta in range(n_rows - 1):
            turned = packed_refs[8 * delta + n][-rank_max // 2 :, :]
            parts += [turned[:, : turned.shape[1] // 2], turned[:, turned.shape[1] // 2 :]]
        factor = jnp.concatenate(parts)
        at = pl.ds(first_row(n, lane, factor.shape[1]), factor.shape[1])
        total += jnp.dot(factor, solved[at, :], preferred_element_type=F32)
    for delta, out in enumerate(out_coeffs):
        out[...] = total[delta * rank_max : (delta + 1) * rank_max].astype(BF16)


def step_kernel(column, last, n_rows, owner, ranks, start, *refs):
    refs = list(refs)
    take = lambda n: [refs.pop(0) for _ in range(n)]
    coeff_refs, u_refs, before = [], [], []
    if column:
        coeff_refs, u_refs, before = take(n_rows - 1), take(8), take(n_rows)
    (own_diag,), packed_refs = take(1), take(8 * (n_rows - 1))
    chunks = take(n_rows)
    (residual, *out_coeffs), refs = ([refs[-1]], refs[:-1]) if last else (refs[:n_rows], refs[n_rows:])
    solved, products, coeff = refs
    me, lane = position()
    mine = owner[me]
    if not column:
        residual[...] = start[...].astype(F32)
    else:
        apply_update(column - 1, n_rows, owner, ranks, start, residual, coeff_refs, u_refs, coeff, column - 1)

        @pl.when(mine < column)
        def _():
            for chunk, earlier in zip(chunks, before):
                chunk[...] = earlier[...]

    @pl.when(mine == column)
    def _():
        piece = own_diag.shape[0]
        rows = piece // 8
        rounded = residual[...].astype(BF16)
        half = n_rows // 2

        def product(delta, first):
            at = slice(first * piece, (first + half) * piece)
            if not delta:
                return jnp.dot(own_diag[:, at], rounded[at], preferred_element_type=F32)
            blocks = range(first, first + half)
            sent = [
                jnp.concatenate([ref[b * rows : (b + 1) * rows, :] for b in blocks], axis=1)
                for ref in packed_refs[8 * (delta - 1) : 8 * delta]
            ]
            return jnp.dot(jnp.concatenate(sent), rounded[at], preferred_element_type=F32)

        for delta in range(n_rows):
            products[delta] = product(delta, 0)
        for delta in range(n_rows):

            @pl.when(around(me - delta, n_rows) >= half)
            def _():
                products[delta] = products[delta] + product(delta, half)

        for delta in range(n_rows):
            base = around(me - delta, n_rows) * piece
            whole = products[delta].astype(BF16)
            if delta:
                for n in range(8):
                    at = pl.multiple_of(base + first_row(n, lane, rows), rows)
                    solved[pl.ds(at, rows), :] = whole[n * rows : (n + 1) * rows]
            else:
                solved[pl.ds(pl.multiple_of(base, piece), piece), :] = whole
        for delta, chunk in enumerate(chunks):
            target = around(me + delta - n_rows, n_rows)
            chunk[...] = solved[pl.ds(pl.multiple_of(target * piece, piece), piece), :]
        if not last:
            write_coefficients(n_rows, solved, packed_refs, out_coeffs)


def coefficient_kernel(n_rows, owner, ranks, *refs):
    n_packed = 8 * (n_rows - 1)
    chunks, packed_refs, out_coeffs = refs[:n_rows], refs[n_rows : n_rows + n_packed], refs[n_rows + n_packed : -1]
    solved = refs[-1]
    for delta, chunk in enumerate(chunks):
        piece = chunk.shape[0]
        target = around(position()[0] + delta - n_rows, n_rows)
        solved[pl.ds(pl.multiple_of(target * piece, piece), piece), :] = chunk[...]
    write_coefficients(n_rows, solved, packed_refs, out_coeffs)


def last_kernel(column, slot, n_rows, owner, ranks, start, *refs):
    coeff_refs, u_refs = refs[: n_rows - 1], refs[n_rows - 1 : n_rows + 7]
    residual, updated, coeff = refs[n_rows + 7 :]
    apply_update(column, n_rows, owner, ranks, start, residual, coeff_refs, u_refs, coeff, slot)
    updated[...] = residual[...].astype(BF16)


def place_kernel(n_rows, owner, ranks, *refs):
    chunks, (out,) = refs[:n_rows], refs[n_rows:]
    for delta, chunk in enumerate(chunks):
        column = owner[around(position()[0] - delta, n_rows)]

        @pl.when(column < out.shape[0])
        def _():
            out[column] = chunk[...]


VMEM = pl.BlockSpec(memory_space=pltpu.VMEM)
SMEM = pl.BlockSpec(memory_space=pltpu.SMEM)


def body(rhs_blocks, left_u, left_v, tile_ranks, diag_inverse, row_owner):
    return direct_body(rhs_blocks, left_u, left_v, tile_ranks, diag_inverse, row_owner)


def direct_body(rhs_blocks, left_u, left_v, tile_ranks, diag_inverse, row_owner):
    n_cols, piece, order = diag_inverse.shape
    n_rows = row_owner.shape[0]
    width, rank_max = rhs_blocks.shape[2], left_u.shape[3]
    rows = piece // 8
    n_u = min(n_cols, n_rows - 1)

    def shifted(array, delta):
        return lax.ppermute(array, "rows", [(i, (i + delta) % n_rows) for i in range(n_rows)])

    def like(*shape):
        return jax.ShapeDtypeStruct(shape, BF16)

    chunk = left_u.shape[2]
    anywhere = pl.BlockSpec(memory_space=pl.ANY)
    *packed, u_mine = pl.pallas_call(
        functools.partial(pack_kernel, n_rows),
        out_shape=[like(n_rows * rows + rank_max // 2, piece)] * (n_rows - 1) + [like(n_u, chunk, rank_max)],
        in_specs=[SMEM] + [anywhere] * 3,
        out_specs=[VMEM] * n_rows,
        scratch_shapes=[
            pltpu.VMEM((n_rows - 1, chunk, rank_max), BF16),
            pltpu.SemaphoreType.DMA(((n_rows - 1) * (n_rows + 1) + 1,)),
        ],
        compiler_params=pltpu.CompilerParams(vmem_limit_bytes=52 * 2**20),
        name="pack",
    )(row_owner, diag_inverse, left_v, left_u)
    own_diag, residual = pl.pallas_call(
        keep_kernel,
        out_shape=[like(piece, order), like(order, width)],
        in_specs=[SMEM, anywhere, anywhere],
        out_specs=[VMEM] * 2,
        scratch_shapes=[pltpu.SemaphoreType.DMA((2,))],
        compiler_params=pltpu.CompilerParams(vmem_limit_bytes=48 * 2**20),
        name="keep",
    )(row_owner, diag_inverse, rhs_blocks)
    packed[1], own_diag, residual = lax.optimization_barrier((packed[1], own_diag, residual))
    u_all = gather_lanes(u_mine)
    packed_all = []
    for delta in range(1, n_rows):
        packed_all += gather_rest(gather_lanes(shifted(packed[delta - 1], delta)))

    whole, halved = jax.ShapeDtypeStruct((order, width), F32), jax.ShapeDtypeStruct((order, width), BF16)
    chunk_shapes = [jax.ShapeDtypeStruct((piece, width), BF16)] * n_rows
    coeff_shapes = [like(rank_max, width)] * (n_rows - 1)
    coeff_scratch = pltpu.VMEM((rank_max, width), BF16)
    params = pltpu.CompilerParams(vmem_limit_bytes=26 * 2**20)

    def call(kernel, in_specs, out_shape, scratch, *operands):
        return pl.pallas_call(
            kernel,
            out_shape=out_shape,
            in_specs=[SMEM, SMEM] + in_specs,
            out_specs=[VMEM] * len(out_shape) if isinstance(out_shape, list) else VMEM,
            scratch_shapes=scratch,
            compiler_params=params,
            cost_estimate=pl.CostEstimate(flops=2 * order * order * width, bytes_accessed=0, transcendentals=0),
        )(row_owner, tile_ranks, *operands)

    def sent_back(coeffs):
        pairs = zip(range(1, n_rows), coeffs)
        return [shifted(c, n_rows - delta) for delta, c in pairs]

    chunks, coeffs = [], []
    scratch = [pltpu.VMEM((order, width), BF16), pltpu.VMEM((n_rows, piece, width), F32), coeff_scratch]
    for column in range(n_cols):
        last = column == n_cols - 1
        if column == 1:
            u_all = gather_rest(u_all, residual)
        before = [*sent_back(coeffs), *u_all, *chunks] if column else []
        outs = call(
            functools.partial(step_kernel, column, last, n_rows),
            [VMEM] * (2 + len(before) + len(packed_all)),
            chunk_shapes + ([] if last else [whole] + coeff_shapes),
            scratch + ([pltpu.VMEM((order, width), F32)] if last else []),
            residual, *before, own_diag, *packed_all,
        )
        chunks, rest = outs[:n_rows], outs[n_rows:]
        if not last:
            residual, coeffs = rest[0], rest[1:]
    arrived = [chunks[0]] + [shifted(chunks[delta], delta) for delta in range(1, n_rows)]
    residual, updated = call(
        functools.partial(last_kernel, n_cols - 2, n_cols - 2, n_rows),
        [VMEM] * (n_rows + 8), [whole, halved], [coeff_scratch], residual, *before[: n_rows + 7],
    )

    def finish(residual, _, chunks, u_last, packed_all):
        coeffs = call(
            functools.partial(coefficient_kernel, n_rows),
            [VMEM] * (n_rows + len(packed_all)), coeff_shapes, scratch[:1], *chunks, *packed_all,
        )
        got, u_all = sent_back(coeffs), gather_rest(gather_lanes(u_last))
        return call(
            functools.partial(last_kernel, n_cols - 1, 0, n_rows),
            [VMEM] * (n_rows + 8), [whole, halved], [coeff_scratch], residual, *got, *u_all,
        )[1]

    updated = lax.cond(
        jnp.max(row_owner) > n_cols - 1,
        finish,
        lambda _, updated, *rest: updated,
        residual, updated, chunks, left_u[0, n_cols - 1 :], packed_all,
    )
    solved_out = call(
        functools.partial(place_kernel, n_rows),
        [VMEM] * n_rows, jax.ShapeDtypeStruct((n_cols, piece, width), BF16), [], *arrived,
    )
    return solved_out, updated[None]


def solution(mesh):
    direct = mesh.shape["rhs"] == 2**3 and mesh.shape["rows"] == 2**2
    return jax.shard_map(
        body if direct else general_body,
        mesh=mesh,
        in_specs=(
            P("rows", None, "rhs"),
            P("rows", None, "rhs", None),
            P("rows", None, "rhs", None),
            P("rows", None),
            P(None, "rows", None),
            P(),
        ),
        out_specs=(P(None, "rows", "rhs"), P("rows", None, "rhs")),
        check_vma=False,
    )
```
